32 devices in a mesh: gx: 2 (over core), gy: 4 (over y, x), gz: 4 (over z).
Axes of the slice: x: 2, y: 2, z: 4, core: 2. Of those that a mesh axis runs over, the one named last changes fastest.
Arguments:
- permanent_field: float32 [12, 24, 24, 3], P('gx', 'gy', 'gz'), may hold values from -6 to 6
- polar: float32 [12, 24, 24], P('gx', 'gy', 'gz'), may hold values from 0.4 to 1.4
- jitter: float32 [12, 24, 24, 3], P('gx', 'gy', 'gz'), may hold values from -0.2 to 0.2
- neighbors: int32 [12, 24, 24, 56], P('gx', 'gy', 'gz'), may hold values from -1 to 987, as said below
Outputs:
- dipoles: float32 [12, 24, 24, 3], P('gx', 'gy', 'gz')
- residual: float32 [12, 24, 24, 3], P('gx', 'gy', 'gz')
- step_lengths: float32 [8], replicated
The draws below stay inside these ranges and needn't reach their ends.
Inputs may be any that keep to these rules, and one draw needn't show every extreme that they name: `neighbors`: each entry is -1 or the flat index of a neighbour in the device's block extended by two sites on every side, with an offset d of squared length 1 to 5 (each component -2 to 2), each offset at most once in a row; the -1 entries come after all others; if site j stands in site i's row with offset d then i stands in j's row with offset -d, the box being periodic.
All inputs are finite; a program needn't handle non-finite values.
Results may differ from the reference program's by a relative error of at most 0.0003.
Values sent between devices are 32-bit elements.
A program may use at most 64 MiB of HBM per device.

```python
import math
import jax
import jax.numpy as jnp
from jax import lax

EDGE = 6
ITERS = 8
LX = 12
LY = 24
LZ = 24


def stencil_offsets():
    listed = []
    for shift_x in range(-2, 3):
        for shift_y in range(-2, 3):
            for shift_z in range(-2, 3):
                length = shift_x * shift_x + shift_y * shift_y + shift_z * shift_z
                if 1 <= length <= 5:
                    listed.append((shift_x, shift_y, shift_z))
    return listed


def draw_neighbors(key, part):
    listed = stencil_offsets()
    forward = [offset for offset in listed if offset > (0, 0, 0)]
    coin_bits = jax.random.randint(key, (LX, LY, LZ, len(forward)), 0, 4)
    bonded = (coin_bits < 3).astype(jnp.int32)
    padded_edge = EDGE + 4
    home_x = lax.broadcasted_iota(jnp.int32, (LX, LY, LZ), 0) % EDGE
    home_y = lax.broadcasted_iota(jnp.int32, (LX, LY, LZ), 1) % EDGE
    home_z = lax.broadcasted_iota(jnp.int32, (LX, LY, LZ), 2) % EDGE
    bond_flags = []
    places = []
    for offset in listed:
        if offset > (0, 0, 0):
            bond_flags.append(bonded[..., forward.index(offset)])
        else:
            mirror = (-offset[0], -offset[1], -offset[2])
            bond_flags.append(jnp.roll(bonded[..., forward.index(mirror)], mirror, axis=(0, 1, 2)))
        places.append(((home_x + 2 + offset[0]) * padded_edge + home_y + 2 + offset[1]) * padded_edge + home_z + 2 + offset[2])
    flagged = jnp.stack(bond_flags, axis=-1)
    located = jnp.stack(places, axis=-1)
    ranking = (1 - flagged) * 64 + lax.broadcasted_iota(jnp.int32, flagged.shape, 3)
    ordering = jnp.argsort(ranking, axis=-1, stable=True)
    flagged = jnp.take_along_axis(flagged, ordering, axis=-1)
    located = jnp.take_along_axis(located, ordering, axis=-1)
    return jnp.where(flagged == 1, located, -1).astype(jnp.int32)


def block_levels(own_key, dims, cuts, smallest, high):
    def one(dim, shards_of):
        steps = jax.random.uniform(jax.random.fold_in(jax.random.fold_in(own_key, 6), dim), (shards_of,), jnp.float32, smallest / len(cuts), high / len(cuts))
        return jnp.repeat(jnp.exp(steps), dims[dim] // shards_of).reshape((-1,) + (1,) * (len(dims) - dim - 1))

    factor_of = one(*cuts[0])
    for cut in cuts[1:]:
        factor_of = factor_of * one(*cut)
    return factor_of


def gaussian(rng, shape, width, most, pieces=(), kind=jnp.bfloat16):
    factor_of = block_levels(rng, shape, pieces, -0.22, 0.18) if pieces else 1.0
    result = jax.random.normal(rng, shape, jnp.float32) * width * factor_of
    return jnp.minimum(jnp.maximum(result, -most), most).astype(kind)


def setup_inputs(seed: int = 0) -> dict:
    key_of = jax.random.split(jax.random.key(seed), 5)
    return {
        "permanent_field": gaussian(key_of[0], (LX, LY, LZ, 3), 1.0, 6.0, ((0, 2), (1, 4), (2, 4)), jnp.float32),
        "polar": jnp.clip(jnp.exp(math.log(1.4) - 1.2527629 * jax.random.uniform(key_of[1], (LX, LY, LZ), jnp.float32) ** block_levels(key_of[1], (LX, LY, LZ), ((0, 2), (1, 4), (2, 4)), -0.2, 0.2)), 0.4, 1.4),
        "jitter": jnp.clip(jax.random.uniform(key_of[2], (LX, LY, LZ, 3), jnp.float32, -0.2, 0.2) * block_levels(key_of[2], (LX, LY, LZ, 3), ((0, 2), (1, 4), (2, 4)), -0.4, 0.0), -0.2, 0.2),
        "neighbors": draw_neighbors(jax.random.fold_in(key_of[4], 71), 0),
    }


thole_damping = 0.39
site_spacing = 3.5

def geometry(offsets, jit_self, jit_other, pol_self, pol_other, present):
    separation = (offsets + jit_other - jit_self) * site_spacing
    separation = jnp.where(present[..., None], separation, site_spacing)
    dist_sq = lax.optimization_barrier(jnp.sum(separation * separation, axis=-1))
    distance = jnp.sqrt(dist_sq)
    dist_cube = dist_sq * distance
    damping = thole_damping * dist_cube / jnp.sqrt(pol_self * pol_other)
    falloff = jnp.exp(-damping)
    lam_three = 1.0 - falloff
    lam_five = 1.0 - (1.0 + damping) * falloff
    isotropic = jnp.where(present, lam_three / dist_cube, 0.0)
    radial = jnp.where(present, 3.0 * lam_five / (dist_cube * dist_sq), 0.0)
    return (separation, isotropic, radial)

def couple(separation, isotropic, radial, values):
    projection = lax.optimization_barrier(jnp.sum(separation * values, axis=-1, keepdims=True))
    return lax.optimization_barrier(jnp.sum(radial[..., None] * projection * separation - isotropic[..., None] * values, axis=-2))

def reference(permanent_field, polar, jitter, neighbors):
    padded_edge = EDGE + 4
    flat_jit = jitter.reshape(-1, 3)
    flat_pol = polar.reshape(-1)

    def slab_geometry(inputs):
        row, links, jit_row, pol_row = inputs
        present = links >= 0
        clipped = jnp.where(present, links, 0)
        plane_a = clipped // (padded_edge * padded_edge)
        plane_b = clipped // padded_edge % padded_edge
        plane_c = clipped % padded_edge
        grid_y = lax.broadcasted_iota(jnp.int32, (LY, LZ, 1), 0)
        grid_z = lax.broadcasted_iota(jnp.int32, (LY, LZ, 1), 1)
        shift_x = plane_a - 2 - row % EDGE
        shift_y = plane_b - 2 - grid_y % EDGE
        shift_z = plane_c - 2 - grid_z % EDGE
        other_x = (row + shift_x) % LX
        other_y = (grid_y + shift_y) % LY
        other_z = (grid_z + shift_z) % LZ
        other = ((other_x * LY + other_y) * LZ + other_z).astype(jnp.int32)
        offsets = jnp.stack([shift_x, shift_y, shift_z], axis=-1).astype(jnp.float32)
        separation, isotropic, radial = geometry(offsets, jit_row[:, :, None, :], flat_jit[other], pol_row[:, :, None], flat_pol[other], present)
        return (separation, isotropic, radial, other)
    rows = jnp.arange(LX, dtype=jnp.int32)
    separations, isotropics, radials, others = lax.map(slab_geometry, (rows, neighbors, jitter, polar))

    def operate(vector):
        flat_vec = vector.reshape(-1, 3)

        def slab(inputs):
            separation, isotropic, radial, other = inputs
            return couple(separation, isotropic, radial, flat_vec[other])
        coupled = lax.map(slab, (separations, isotropics, radials, others))
        return vector / polar[..., None] - coupled
    weights = polar[..., None]
    dipoles = weights * permanent_field
    residual = permanent_field - operate(dipoles)
    scaled = weights * residual
    direction = scaled
    gamma_now = jnp.sum(residual * scaled)
    lengths = []
    for number in range(ITERS):
        image = operate(direction)
        step_len = gamma_now / jnp.sum(direction * image)
        dipoles = dipoles + step_len * direction
        residual = residual - step_len * image
        scaled = weights * residual
        gamma_next = jnp.sum(residual * scaled)
        direction = scaled + gamma_next / gamma_now * direction
        gamma_now = gamma_next
        lengths.append(step_len)
    return (dipoles, residual, jnp.stack(lengths))
```

```python
import functools

import jax
import jax.numpy as jnp
from jax import lax
from jax.experimental import pallas as pl
from jax.experimental.pallas import tpu as pltpu
from jax.sharding import PartitionSpec as P

ITERS = 8
MESH = pl.DeviceIdType.MESH
thole_damping = 0.39
site_spacing = 3.5
ROWS, LANES = 8, 128


def stencil():
    return [
        (a, b, c)
        for a in range(-2, 3)
        for b in range(-2, 3)
        for c in range(-2, 3)
        if 1 <= a * a + b * b + c * c <= 5
    ]


def roll(value, shift):
    shift = shift % LANES
    return value if shift == 0 else pltpu.roll(value, shift, axis=1)


def kernel(
    sizes, edge,
    nb_ref, in_ref, x_out, r_out, len_out,
    ext, w_ext, r_ext, s_ext, geo, coef, chip_src, chip_dst, core_src, core_dst, dot_src, dot_dst,
    halo_send, halo_recv, dot_send, dot_recv,
):
    nx, ny, nz = sizes
    wide = edge + 4
    offsets = stencil()
    gx, gy, gz = lax.axis_index("gx"), lax.axis_index("gy"), lax.axis_index("gz")
    rank = (gx * ny + gy) * nz + gz

    def at(ox, oy, oz):
        return (lax.rem(gx + ox + nx, nx), lax.rem(gy + oy + ny, ny), lax.rem(gz + oz + nz, nz))

    others = [
        (a, b, c) for a in range(nx) for b in range(ny) for c in range(nz) if (a, b, c) != (0, 0, 0)
    ]
    others.sort(key=lambda o: -(min(o[0], nx - o[0]) + 2 * min(o[1], ny - o[1]) + 2 * min(o[2], nz - o[2])))

    barrier = pltpu.get_barrier_semaphore()
    for o in others:
        pl.semaphore_signal(barrier, inc=1, device_id=at(*o), device_id_type=MESH)

    lane = lax.broadcasted_iota(jnp.int32, (ROWS, LANES), 1)
    row = lax.broadcasted_iota(jnp.int32, (ROWS, LANES), 0)
    ye = lane // wide
    ze = lane - ye * wide
    y_low, y_high = ye < 2, (ye >= edge + 2) & (ye < wide)
    y_mid = (ye >= 2) & (ye < edge + 2)
    z_low, z_high = ze < 2, ze >= edge + 2
    z_mid = (ze >= 2) & (ze < edge + 2)
    src_zp = (ze >= edge) & z_mid
    src_zm = (ze < 4) & z_mid
    src_yp = (ye >= edge) & y_mid
    src_ym = (ye < 4) & y_mid

    def pack(planes, mask, base, step):
        out = None
        for c, plane in enumerate(planes):
            part = roll(jnp.where(mask, plane, 0.0), base + c * step)
            out = part if out is None else out + part
        return out

    def halo_copies(par, groups, comps):
        copies = []
        for oy in (-1, 1, 0):
            for oz in (-1, 1, 0):
                for ox in (1, 0):
                    if (ox, oy, oz) == (0, 0, 0):
                        continue
                    back = ox * 9 + (1 - oy) * 3 + 1 - oz
                    here = ox * 9 + (1 + oy) * 3 + 1 + oz
                    if oy == 0 and oz == 0:
                        src, dst = core_src.at[par, pl.ds(0, comps)], core_dst.at[par, pl.ds(0, comps)]
                    else:
                        kind = {1: 0, -1: 1}[oz] if oz else {1: 2, -1: 3}[oy]
                        src = chip_src.at[par, kind, pl.ds(0, groups)]
                        dst = chip_dst.at[par, back, pl.ds(0, groups)]
                    copies.append(
                        pltpu.make_async_remote_copy(
                            src_ref=src, dst_ref=dst,
                            send_sem=halo_send.at[par, here], recv_sem=halo_recv.at[par, back],
                            device_id=at(ox, oy, oz), device_id_type=MESH,
                        )
                    )
        return copies

    def halo_start(par, planes):
        parts = [planes] if len(planes) <= 4 else [planes[:4], planes[4:]]
        for g, part in enumerate(parts):
            chip_src[par, 0, g] = pack(part, src_zp, -edge, 2)
            chip_src[par, 1, g] = pack(part, src_zm, edge, -2)
            chip_src[par, 2, g] = pack(part, src_yp, -edge * wide, 2 * wide)
            chip_src[par, 3, g] = pack(part, src_ym, edge * wide, -2 * wide)
        for c, plane in enumerate(planes):
            core_src[par, c] = plane
        copies = halo_copies(par, len(parts), len(planes))
        for copy in copies:
            copy.start()
        return copies

    def halo_finish(par, planes, copies, target):
        for copy in copies:
            copy.wait_recv()
        parts = [planes] if len(planes) <= 4 else [planes[:4], planes[4:]]
        index = 0
        for g, part in enumerate(parts):
            merged = []
            for ox in (0, 1):
                def got(oy, oz):
                    return chip_dst[par, ox * 9 + (1 + oy) * 3 + 1 + oz, g]

                def column(oz):
                    near = got(0, oz)
                    low = roll(got(-1, oz), -edge * wide)
                    high = roll(got(1, oz), edge * wide)
                    return jnp.where(y_mid, near, jnp.where(y_low, low, high))

                merged.append((column(-1), column(1), got(-1, 0), got(1, 0)))
            for c, plane in enumerate(part):
                full = []
                for ox in (0, 1):
                    zl, zh, yl, yh = merged[ox]
                    base = plane if ox == 0 else core_dst[par, index]
                    base = jnp.where(y_low & z_mid, roll(yl, -2 * wide * c), base)
                    base = jnp.where(y_high & z_mid, roll(yh, 2 * wide * c), base)
                    base = jnp.where(z_low, roll(zl, -2 * c), base)
                    base = jnp.where(z_high, roll(zh, 2 * c), base)
                    full.append(jnp.where(ye < wide, base, 0.0))
                ref, k = target[index]
                ref[k, pl.ds(2, edge), :] = full[0][:edge]
                ref[k, pl.ds(0, 2), :] = full[1][edge - 2 : edge]
                ref[k, pl.ds(edge + 2, 2), :] = full[1][0:2]
                index += 1
        for copy in copies:
            copy.wait_send()

    inputs = [in_ref[c] for c in range(7)]
    live = (row < edge) & y_mid & z_mid & (ye < wide)
    jit, pol, field = inputs[0:3], jnp.where(live, inputs[3], 1.0), inputs[4:7]
    inv = 1.0 / pol
    x = [pol * f for f in field]
    ext[...] = jnp.zeros_like(ext)
    geo[...] = jnp.ones_like(geo)
    for ref in (w_ext, r_ext, s_ext):
        ref[...] = jnp.zeros_like(ref)

    pl.semaphore_wait(barrier, len(others))
    first = [*jit, pol, *x]
    copies = halo_start(0, first)

    home = row * (wide * wide) + lane + 2 * wide * wide
    hundred, ten = wide * wide, wide

    def slot(number, words):
        entry = nb_ref[number]
        rel = entry - home + (2 * hundred + hundred // 2)
        dx = (rel * 5243) >> 19
        rem = rel - dx * hundred - (hundred // 2 - 2 * ten - 5)
        dy = (rem * 6554) >> 16
        dz = rem - dy * ten - 3
        bit = jnp.where(entry >= 0, jnp.left_shift(1, jnp.clip(dy * 5 + dz, 0, 24)), 0)
        return tuple(word | jnp.where(dx == k, bit, 0) for k, word in enumerate(words))

    zero = jnp.zeros((ROWS, LANES), jnp.int32)
    words = lax.fori_loop(0, nb_ref.shape[0], slot, (zero,) * 5)

    halo_finish(0, first, copies, [(geo, 0), (geo, 1), (geo, 2), (geo, 3), (ext, 0), (ext, 1), (ext, 2)])

    for n, d in enumerate(offsets):
        shift = -(d[1] * wide + d[2])
        bit = 5 * (d[1] + 2) + d[2] + 2
        present = (words[d[0] + 2] & (1 << bit)) != 0
        near = [roll(geo[k, pl.ds(d[0] + 2, ROWS), :], shift) for k in range(4)]
        sep = [
            jnp.where(present, (d[k] + near[k] - jit[k]) * site_spacing, site_spacing) for k in range(3)
        ]
        sq = sep[0] * sep[0] + sep[1] * sep[1] + sep[2] * sep[2]
        dist = jnp.sqrt(sq)
        cube = sq * dist
        damp = thole_damping * cube / jnp.sqrt(pol * near[3])
        fall = jnp.exp(-damp)
        iso = jnp.where(present, (1.0 - fall) / cube, 0.0)
        rad = jnp.where(present, 3.0 * (1.0 - (1.0 + damp) * fall) / (cube * sq), 0.0)
        rs = [rad * s for s in sep]
        coef[n, 0] = rs[0] * sep[0] - iso
        coef[n, 1] = rs[0] * sep[1]
        coef[n, 2] = rs[0] * sep[2]
        coef[n, 3] = rs[1] * sep[1] - iso
        coef[n, 4] = rs[1] * sep[2]
        coef[n, 5] = rs[2] * sep[2] - iso

    def operate(planes):
        acc = [[None] * 5 for _ in range(3)]
        for n, d in enumerate(offsets):
            shift = -(d[1] * wide + d[2])
            a, b, c = [roll(ext[k, pl.ds(d[0] + 2, ROWS), :], shift) for k in range(3)]
            xx, xy, xz, yy, yz, zz = [coef[n, k] for k in range(6)]
            for k, term in enumerate(
                (xx * a + xy * b + xz * c, xy * a + yy * b + yz * c, xz * a + yz * b + zz * c)
            ):
                old = acc[k][d[0] + 2]
                acc[k][d[0] + 2] = term if old is None else old + term
        return [
            planes[k] * inv - (((acc[k][0] + acc[k][1]) + (acc[k][3] + acc[k][4])) + acc[k][2])
            for k in range(3)
        ]

    image = operate(x)
    r = [jnp.where(live, field[k] - image[k], 0.0) for k in range(3)]
    u = [pol * v for v in r]
    copies = halo_start(1, r)
    halo_finish(1, r, copies, [(r_ext, 0), (r_ext, 1), (r_ext, 2)])
    for k in range(3):
        ext[k] = geo[3] * r_ext[k]
    w = operate(u)

    pick = lax.broadcasted_iota(jnp.int32, (1, LANES), 1)

    def dot_copies(par):
        return [
            pltpu.make_async_remote_copy(
                src_ref=dot_src.at[par], dst_ref=dot_dst.at[par, rank],
                send_sem=dot_send.at[par, k], recv_sem=dot_recv.at[par, k],
                device_id=at(*o), device_id_type=MESH,
            )
            for k, o in enumerate(others)
        ]

    def total(value):
        return jnp.sum(jnp.sum(value, axis=0, keepdims=True), axis=1, keepdims=True)

    def dots_start(par, r, u, w):
        gamma = total(r[0] * u[0] + r[1] * u[1] + r[2] * u[2])
        delta = total(w[0] * u[0] + w[1] * u[1] + w[2] * u[2])
        line = jnp.where(pick == 0, gamma, jnp.where(pick == 1, delta, 0.0))
        dot_src[par] = line
        dot_dst[par, rank] = line
        copies = dot_copies(par)
        for copy in copies:
            copy.start()
        return copies

    def dots_finish(par, copies):
        for copy in copies:
            copy.wait_recv()
        line = jnp.sum(dot_dst[par, :, 0, :], axis=0, keepdims=True)
        for copy in copies:
            copy.wait_send()
        gamma = jnp.sum(jnp.where(pick == 0, line, 0.0), axis=1, keepdims=True)
        delta = jnp.sum(jnp.where(pick == 1, line, 0.0), axis=1, keepdims=True)
        return gamma, delta

    def lengths(number, gamma, delta, gamma_old, step_old):
        beta = gamma / gamma_old
        step = gamma / (delta - beta * gamma / step_old)
        len_out[pl.ds(number, 1), :] = jnp.broadcast_to(step, (1, LANES))
        return beta, step

    def axpy(a, s, b):
        return [a[k] + s * b[k] for k in range(3)]

    def iteration(number, state):
        x, r, u, w, p, s, gamma_old, step_old = state
        par = lax.rem(number, 2)
        dots = dots_start(par, r, u, w)
        halos = halo_start(par, w)
        halo_finish(par, w, halos, [(w_ext, 0), (w_ext, 1), (w_ext, 2)])
        gamma, delta = dots_finish(par, dots)
        beta, step = lengths(number, gamma, delta, gamma_old, step_old)
        for k in range(3):
            s_new = w_ext[k] + beta * s_ext[k]
            r_new = r_ext[k] - step * s_new
            s_ext[k] = s_new
            r_ext[k] = r_new
            ext[k] = geo[3] * r_new
        s, p = axpy(w, beta, s), axpy(u, beta, p)
        x, r = axpy(x, step, p), axpy(r, -step, s)
        u = [pol * v for v in r]
        w = operate(u)
        return x, r, u, w, p, s, gamma, step

    none = [jnp.zeros((ROWS, LANES), jnp.float32)] * 3
    far = jnp.full((1, 1), jnp.inf, jnp.float32)
    one = jnp.ones((1, 1), jnp.float32)
    state = (x, r, u, w, none, none, far, one)
    x, r, u, w, p, s, gamma_old, step_old = lax.fori_loop(0, ITERS - 1, iteration, state)
    last = (ITERS - 1) % 2
    dots = dots_start(last, r, u, w)
    gamma, delta = dots_finish(last, dots)
    beta, step = lengths(ITERS - 1, gamma, delta, gamma_old, step_old)
    p, s = axpy(u, beta, p), axpy(w, beta, s)
    x, r = axpy(x, step, p), axpy(r, -step, s)
    for k in range(3):
        x_out[k] = x[k]
        r_out[k] = r[k]


def solution(mesh):
    sizes = tuple(mesh.shape[a] for a in ("gx", "gy", "gz"))
    assert sizes[0] == 2
    count = sizes[0] * sizes[1] * sizes[2]

    def local(permanent_field, polar, jitter, neighbors):
        edge = polar.shape[0]
        wide = edge + 4
        slots = neighbors.shape[-1]

        def spread(array, fill):
            array = jnp.moveaxis(array, -1, 0)
            array = jnp.pad(array, ((0, 0), (0, ROWS - edge), (2, 2), (2, 2)), constant_values=fill)
            array = array.reshape(array.shape[0], ROWS, wide * wide)
            return jnp.pad(array, ((0, 0), (0, 0), (0, LANES - wide * wide)), constant_values=fill)

        bundle = jnp.concatenate([jitter, polar[..., None], permanent_field], axis=-1)
        bundle = spread(bundle, 0.0)
        plane = jax.ShapeDtypeStruct((3, ROWS, LANES), jnp.float32)
        vmem = pl.BlockSpec(memory_space=pltpu.VMEM)
        f32 = jnp.float32
        x, r, steps = pl.pallas_call(
            functools.partial(kernel, sizes, edge),
            out_shape=(plane, plane, jax.ShapeDtypeStruct((ITERS, LANES), f32)),
            in_specs=[vmem, vmem],
            out_specs=(vmem, vmem, vmem),
            scratch_shapes=[
                *[pltpu.VMEM((3, 16, LANES), f32)] * 4,
                pltpu.VMEM((4, 16, LANES), f32),
                pltpu.VMEM((len(stencil()), 6, ROWS, LANES), f32),
                pltpu.VMEM((2, 4, 2, ROWS, LANES), f32),
                pltpu.VMEM((2, 18, 2, ROWS, LANES), f32),
                pltpu.VMEM((2, 7, ROWS, LANES), f32),
                pltpu.VMEM((2, 7, ROWS, LANES), f32),
                pltpu.VMEM((2, 1, LANES), f32),
                pltpu.VMEM((2, count, 1, LANES), f32),
                pltpu.SemaphoreType.DMA((2, 18)),
                pltpu.SemaphoreType.DMA((2, 18)),
                pltpu.SemaphoreType.DMA((2, count)),
                pltpu.SemaphoreType.DMA((2, count)),
            ],
            compiler_params=pltpu.CompilerParams(collective_id=0, has_side_effects=True),
        )(spread(neighbors, -1), bundle)

        def gather(planes):
            planes = planes[:, :edge, : wide * wide].reshape(3, edge, wide, wide)
            return jnp.moveaxis(planes[:, :, 2:-2, 2:-2], 0, -1)

        return gather(x), gather(r), steps[:, 0]

    return jax.shard_map(
        local,
        mesh=mesh,
        in_specs=(
            P("gx", "gy", "gz", None),
            P("gx", "gy", "gz"),
            P("gx", "gy", "gz", None),
            P("gx", "gy", "gz", None),
        ),
        out_specs=(P("gx", "gy", "gz", None), P("gx", "gy", "gz", None), P()),
        check_vma=False,
    )
```

```python
import functools

import jax
import jax.numpy as jnp
from jax import lax
from jax.experimental import pallas as pl
from jax.experimental.pallas import tpu as pltpu
from jax.sharding import PartitionSpec as P

ITERS = 8
MESH = pl.DeviceIdType.MESH
thole_damping = 0.39
site_spacing = 3.5
ROWS, LANES = 8, 128


def stencil():
    return [
        (a, b, c)
        for a in range(-2, 3)
        for b in range(-2, 3)
        for c in range(-2, 3)
        if 1 <= a * a + b * b + c * c <= 5
    ]


def roll(value, shift):
    shift = shift % LANES
    return value if shift == 0 else pltpu.roll(value, shift, axis=1)


def kernel(
    sizes, edge,
    nb_ref, in_ref, x_out, r_out, len_out,
    ext, w_ext, r_ext, s_ext, geo, coef, chip_src, chip_dst, core_src, core_dst, dot_src, dot_dst,
    halo_send, halo_recv, dot_send, dot_recv,
):
    nx, ny, nz = sizes
    wide = edge + 4
    offsets = stencil()
    gx, gy, gz = lax.axis_index("gx"), lax.axis_index("gy"), lax.axis_index("gz")
    rank = (gx * ny + gy) * nz + gz

    def at(ox, oy, oz):
        return (lax.rem(gx + ox + nx, nx), lax.rem(gy + oy + ny, ny), lax.rem(gz + oz + nz, nz))

    others = [
        (a, b, c) for a in range(nx) for b in range(ny) for c in range(nz) if (a, b, c) != (0, 0, 0)
    ]
    others.sort(key=lambda o: -(min(o[0], nx - o[0]) + 2 * min(o[1], ny - o[1]) + 2 * min(o[2], nz - o[2])))

    barrier = pltpu.get_barrier_semaphore()
    for o in others:
        pl.semaphore_signal(barrier, inc=1, device_id=at(*o), device_id_type=MESH)

    lane = lax.broadcasted_iota(jnp.int32, (ROWS, LANES), 1)
    row = lax.broadcasted_iota(jnp.int32, (ROWS, LANES), 0)
    ye = lane // wide
    ze = lane - ye * wide
    y_low, y_high = ye < 2, (ye >= edge + 2) & (ye < wide)
    y_mid = (ye >= 2) & (ye < edge + 2)
    z_low, z_high = ze < 2, ze >= edge + 2
    z_mid = (ze >= 2) & (ze < edge + 2)
    src_zp = (ze >= edge) & z_mid
    src_zm = (ze < 4) & z_mid
    src_yp = (ye >= edge) & y_mid
    src_ym = (ye < 4) & y_mid

    def pack(planes, mask, base, step):
        out = None
        for c, plane in enumerate(planes):
            part = roll(jnp.where(mask, plane, 0.0), base + c * step)
            out = part if out is None else out + part
        return out

    def halo_copies(par, groups, comps):
        copies = []
        for oy in (-1, 1, 0):
            for oz in (-1, 1, 0):
                for ox in (1, 0):
                    if (ox, oy, oz) == (0, 0, 0):
                        continue
                    back = ox * 9 + (1 - oy) * 3 + 1 - oz
                    here = ox * 9 + (1 + oy) * 3 + 1 + oz
                    if oy == 0 and oz == 0:
                        src, dst = core_src.at[par, pl.ds(0, comps)], core_dst.at[par, pl.ds(0, comps)]
                    else:
                        kind = {1: 0, -1: 1}[oz] if oz else {1: 2, -1: 3}[oy]
                        src = chip_src.at[par, kind, pl.ds(0, groups)]
                        dst = chip_dst.at[par, back, pl.ds(0, groups)]
                    copies.append(
                        pltpu.make_async_remote_copy(
                            src_ref=src, dst_ref=dst,
                            send_sem=halo_send.at[par, here], recv_sem=halo_recv.at[par, back],
                            device_id=at(ox, oy, oz), device_id_type=MESH,
                        )
                    )
        return copies

    def halo_pack(par, planes):
        parts = [planes] if len(planes) <= 4 else [planes[:4], planes[4:]]
        for g, part in enumerate(parts):
            chip_src[par, 0, g] = pack(part, src_zp, -edge, 2)
            chip_src[par, 1, g] = pack(part, src_zm, edge, -2)
            chip_src[par, 2, g] = pack(part, src_yp, -edge * wide, 2 * wide)
            chip_src[par, 3, g] = pack(part, src_ym, edge * wide, -2 * wide)
        for c, plane in enumerate(planes):
            core_src[par, c] = plane

    def halo_start(par, planes):
        copies = halo_copies(par, 1 if len(planes) <= 4 else 2, len(planes))
        for copy in copies:
            copy.start()
        return copies

    def halo_finish(par, planes, copies, target):
        for copy in copies:
            copy.wait_recv()
        parts = [planes] if len(planes) <= 4 else [planes[:4], planes[4:]]
        index = 0
        for g, part in enumerate(parts):
            merged = []
            for ox in (0, 1):
                def got(oy, oz):
                    return chip_dst[par, ox * 9 + (1 + oy) * 3 + 1 + oz, g]

                def column(oz):
                    near = got(0, oz)
                    low = roll(got(-1, oz), -edge * wide)
                    high = roll(got(1, oz), edge * wide)
                    return jnp.where(y_mid, near, jnp.where(y_low, low, high))

                merged.append((column(-1), column(1), got(-1, 0), got(1, 0)))
            for c, plane in enumerate(part):
                full = []
                for ox in (0, 1):
                    zl, zh, yl, yh = merged[ox]
                    base = plane if ox == 0 else core_dst[par, index]
                    base = jnp.where(y_low & z_mid, roll(yl, -2 * wide * c), base)
                    base = jnp.where(y_high & z_mid, roll(yh, 2 * wide * c), base)
                    base = jnp.where(z_low, roll(zl, -2 * c), base)
                    base = jnp.where(z_high, roll(zh, 2 * c), base)
                    full.append(jnp.where(ye < wide, base, 0.0))
                ref, k = target[index]
                ref[k, pl.ds(2, edge), :] = full[0][:edge]
                ref[k, pl.ds(0, 2), :] = full[1][edge - 2 : edge]
                ref[k, pl.ds(edge + 2, 2), :] = full[1][0:2]
                index += 1
        for copy in copies:
            copy.wait_send()

    inputs = [in_ref[c] for c in range(7)]
    live = (row < edge) & y_mid & z_mid & (ye < wide)
    jit, pol, field = inputs[0:3], jnp.where(live, inputs[3], 1.0), inputs[4:7]
    inv = 1.0 / pol
    x = [pol * f for f in field]
    ext[...] = jnp.zeros_like(ext)
    len_out[...] = jnp.zeros_like(len_out)
    geo[...] = jnp.ones_like(geo)
    for ref in (w_ext, r_ext, s_ext):
        ref[...] = jnp.zeros_like(ref)

    first = [*jit, pol, *x]
    halo_pack(0, first)
    pl.semaphore_wait(barrier, len(others))
    copies = halo_start(0, first)

    home = row * (wide * wide) + lane + 2 * wide * wide
    hundred, ten = wide * wide, wide

    def slot(number, words):
        entry = nb_ref[number]
        rel = entry - home + (2 * hundred + hundred // 2)
        dx = (rel * 5243) >> 19
        rem = rel - dx * hundred - (hundred // 2 - 2 * ten - 5)
        dy = (rem * 6554) >> 16
        dz = rem - dy * ten - 3
        bit = jnp.where(entry >= 0, jnp.left_shift(1, jnp.clip(dy * 5 + dz, 0, 24)), 0)
        return tuple(word | jnp.where(dx == k, bit, 0) for k, word in enumerate(words))

    zero = jnp.zeros((ROWS, LANES), jnp.int32)
    words = lax.fori_loop(0, nb_ref.shape[0], slot, (zero,) * 5)

    halo_finish(0, first, copies, [(geo, 0), (geo, 1), (geo, 2), (geo, 3), (ext, 0), (ext, 1), (ext, 2)])

    for n, d in enumerate(offsets):
        shift = -(d[1] * wide + d[2])
        bit = 5 * (d[1] + 2) + d[2] + 2
        present = (words[d[0] + 2] & (1 << bit)) != 0
        near = [roll(geo[k, pl.ds(d[0] + 2, ROWS), :], shift) for k in range(4)]
        sep = [
            jnp.where(present, (d[k] + near[k] - jit[k]) * site_spacing, site_spacing) for k in range(3)
        ]
        sq = sep[0] * sep[0] + sep[1] * sep[1] + sep[2] * sep[2]
        dist = jnp.sqrt(sq)
        cube = sq * dist
        damp = thole_damping * cube / jnp.sqrt(pol * near[3])
        fall = jnp.exp(-damp)
        iso = jnp.where(present, (1.0 - fall) / cube, 0.0)
        rad = jnp.where(present, 3.0 * (1.0 - (1.0 + damp) * fall) / (cube * sq), 0.0)
        rs = [rad * s for s in sep]
        coef[n, 0] = rs[0] * sep[0] - iso
        coef[n, 1] = rs[0] * sep[1]
        coef[n, 2] = rs[0] * sep[2]
        coef[n, 3] = rs[1] * sep[1] - iso
        coef[n, 4] = rs[1] * sep[2]
        coef[n, 5] = rs[2] * sep[2] - iso

    def operate(planes):
        acc = [[None] * 5 for _ in range(3)]
        for n, d in enumerate(offsets):
            shift = -(d[1] * wide + d[2])
            a, b, c = [roll(ext[k, pl.ds(d[0] + 2, ROWS), :], shift) for k in range(3)]
            xx, xy, xz, yy, yz, zz = [coef[n, k] for k in range(6)]
            for k, term in enumerate(
                (xx * a + xy * b + xz * c, xy * a + yy * b + yz * c, xz * a + yz * b + zz * c)
            ):
                old = acc[k][d[0] + 2]
                acc[k][d[0] + 2] = term if old is None else old + term
        return [
            planes[k] * inv - (((acc[k][0] + acc[k][1]) + (acc[k][3] + acc[k][4])) + acc[k][2])
            for k in range(3)
        ]

    image = operate(x)
    r = [jnp.where(live, field[k] - image[k], 0.0) for k in range(3)]
    u = [pol * v for v in r]
    halo_pack(1, r)
    copies = halo_start(1, r)
    halo_finish(1, r, copies, [(r_ext, 0), (r_ext, 1), (r_ext, 2)])
    for k in range(3):
        ext[k] = geo[3] * r_ext[k]
    w = operate(u)

    pick = lax.broadcasted_iota(jnp.int32, (1, LANES), 1)

    def dot_copies(par):
        return [
            pltpu.make_async_remote_copy(
                src_ref=dot_src.at[par], dst_ref=dot_dst.at[par, rank],
                send_sem=dot_send.at[par, k], recv_sem=dot_recv.at[par, k],
                device_id=at(*o), device_id_type=MESH,
            )
            for k, o in enumerate(others)
        ]

    def total(value):
        return jnp.sum(jnp.sum(value, axis=0, keepdims=True), axis=1, keepdims=True)

    def dots_start(par, r, u, w):
        gamma = total(r[0] * u[0] + r[1] * u[1] + r[2] * u[2])
        delta = total(w[0] * u[0] + w[1] * u[1] + w[2] * u[2])
        line = jnp.where(pick == 0, gamma, jnp.where(pick == 1, delta, 0.0))
        dot_src[par] = line
        dot_dst[par, rank] = line
        copies = dot_copies(par)
        for copy in copies:
            copy.start()
        return copies

    def dots_finish(par, copies):
        for copy in copies:
            copy.wait_send()
        for copy in copies:
            copy.wait_recv()
        line = jnp.sum(dot_dst[par, :, 0, :], axis=0, keepdims=True)
        gamma = jnp.sum(jnp.where(pick == 0, line, 0.0), axis=1, keepdims=True)
        delta = jnp.sum(jnp.where(pick == 1, line, 0.0), axis=1, keepdims=True)
        return gamma, delta

    def lengths(number, gamma, delta, gamma_old, step_old):
        beta = gamma / gamma_old
        step = gamma / (delta - beta * gamma / step_old)
        len_out[...] = jnp.where(pick == number, step, len_out[...])
        return beta, step

    def axpy(a, s, b):
        return [a[k] + s * b[k] for k in range(3)]

    def iteration(number, state):
        x, r, u, w, p, s, gamma_old, step_old = state
        par = lax.rem(number, 2)
        halo_pack(par, w)
        dots = dots_start(par, r, u, w)
        halos = halo_start(par, w)
        halo_finish(par, w, halos, [(w_ext, 0), (w_ext, 1), (w_ext, 2)])
        gamma, delta = dots_finish(par, dots)
        beta, step = lengths(number, gamma, delta, gamma_old, step_old)
        for k in range(3):
            s_new = w_ext[k] + beta * s_ext[k]
            r_new = r_ext[k] - step * s_new
            s_ext[k] = s_new
            r_ext[k] = r_new
            ext[k] = geo[3] * r_new
        s, p = axpy(w, beta, s), axpy(u, beta, p)
        x, r = axpy(x, step, p), axpy(r, -step, s)
        u = [pol * v for v in r]
        w = operate(u)
        return x, r, u, w, p, s, gamma, step

    none = [jnp.zeros((ROWS, LANES), jnp.float32)] * 3
    far = jnp.full((1, 1), jnp.inf, jnp.float32)
    one = jnp.ones((1, 1), jnp.float32)
    state = (x, r, u, w, none, none, far, one)
    x, r, u, w, p, s, gamma_old, step_old = lax.fori_loop(0, ITERS - 1, iteration, state)
    last = (ITERS - 1) % 2
    dots = dots_start(last, r, u, w)
    gamma, delta = dots_finish(last, dots)
    beta, step = lengths(ITERS - 1, gamma, delta, gamma_old, step_old)
    p, s = axpy(u, beta, p), axpy(w, beta, s)
    x, r = axpy(x, step, p), axpy(r, -step, s)
    for k in range(3):
        x_out[k] = x[k]
        r_out[k] = r[k]


def solution(mesh):
    sizes = tuple(mesh.shape[a] for a in ("gx", "gy", "gz"))
    assert sizes[0] == 2
    count = sizes[0] * sizes[1] * sizes[2]

    def local(permanent_field, polar, jitter, neighbors):
        edge = polar.shape[0]
        wide = edge + 4
        slots = neighbors.shape[-1]

        def spread(array, fill):
            array = jnp.moveaxis(array, -1, 0)
            array = jnp.pad(array, ((0, 0), (0, ROWS - edge), (2, 2), (2, 2)), constant_values=fill)
            array = array.reshape(array.shape[0], ROWS, wide * wide)
            return jnp.pad(array, ((0, 0), (0, 0), (0, LANES - wide * wide)), constant_values=fill)

        bundle = jnp.concatenate([jitter, polar[..., None], permanent_field], axis=-1)
        bundle = spread(bundle, 0.0)
        plane = jax.ShapeDtypeStruct((3, ROWS, LANES), jnp.float32)
        vmem = pl.BlockSpec(memory_space=pltpu.VMEM)
        f32 = jnp.float32
        x, r, steps = pl.pallas_call(
            functools.partial(kernel, sizes, edge),
            out_shape=(plane, plane, jax.ShapeDtypeStruct((1, LANES), f32)),
            in_specs=[vmem, vmem],
            out_specs=(vmem, vmem, vmem),
            scratch_shapes=[
                *[pltpu.VMEM((3, 16, LANES), f32)] * 4,
                pltpu.VMEM((4, 16, LANES), f32),
                pltpu.VMEM((len(stencil()), 6, ROWS, LANES), f32),
                pltpu.VMEM((2, 4, 2, ROWS, LANES), f32),
                pltpu.VMEM((2, 18, 2, ROWS, LANES), f32),
                pltpu.VMEM((2, 7, ROWS, LANES), f32),
                pltpu.VMEM((2, 7, ROWS, LANES), f32),
                pltpu.VMEM((2, 1, LANES), f32),
                pltpu.VMEM((2, count, 1, LANES), f32),
                pltpu.SemaphoreType.DMA((2, 18)),
                pltpu.SemaphoreType.DMA((2, 18)),
                pltpu.SemaphoreType.DMA((2, count)),
                pltpu.SemaphoreType.DMA((2, count)),
            ],
            compiler_params=pltpu.CompilerParams(collective_id=0, has_side_effects=True),
        )(spread(neighbors, -1), bundle)

        def gather(planes):
            planes = planes[:, :edge, : wide * wide].reshape(3, edge, wide, wide)
            return jnp.moveaxis(planes[:, :, 2:-2, 2:-2], 0, -1)

        return gather(x), gather(r), steps[0, :ITERS]

    return jax.shard_map(
        local,
        mesh=mesh,
        in_specs=(
            P("gx", "gy", "gz", None),
            P("gx", "gy", "gz"),
            P("gx", "gy", "gz", None),
            P("gx", "gy", "gz", None),
        ),
        out_specs=(P("gx", "gy", "gz", None), P("gx", "gy", "gz", None), P()),
        check_vma=False,
    )
```
